256 devices in a mesh: t: 4 (over x), v: 64 (over z, y, core).
Axes of the slice: x: 4, y: 4, z: 8, core: 2. Of those that a mesh axis runs over, the one named last changes fastest.
Arguments:
- hidden_in: bfloat16 [256, 2304], replicated
- seq_lens: int32 [256], replicated
- target: int32 [256], replicated
- g_attn_pre: bfloat16 [2304], replicated
- w_q: bfloat16 [2304, 2048], P(None, 't')
- w_k: bfloat16 [2304, 1024], P(None, 't')
- w_v: bfloat16 [2304, 1024], P(None, 't')
- w_o: bfloat16 [2048, 2304], P('t')
- g_attn_post: bfloat16 [2304], replicated
- g_mlp_pre: bfloat16 [2304], replicated
- w_gate: bfloat16 [2304, 9216], P(None, 't')
- w_up: bfloat16 [2304, 9216], P(None, 't')
- w_down: bfloat16 [9216, 2304], P('t')
- g_mlp_post: bfloat16 [2304], replicated
- g_final: bfloat16 [2304], replicated
- k_cache: bfloat16 [256, 256, 4, 256], P(None, None, 't')
- v_cache: bfloat16 [256, 256, 4, 256], P(None, None, 't')
- embed_table: bfloat16 [256000, 2304], P(('v', 't'))
Outputs:
- output 1: float32 [256], replicated
- output 2: bfloat16 [256, 2304], replicated
All inputs are finite; a program needn't handle non-finite values.
Results may differ from the reference program's by a relative error of at most 0.00723531.
Values sent between devices are 32-bit elements.
A program may use at most 768 MiB of HBM per device.

```python
import jax
import jax.numpy as jnp
from jax import lax

D = 2304
HEADS = 8
KV_HEADS = 4
HEAD = 256
FF = 9216
VOCAB = 256000
TOKENS = 256
CTX = 256

ATTN_CAP = 50.0
FINAL_CAP = 30.0
NORM_EPS = 1e-6
ROPE_BASE = 10000.0


def rms_norm(values, gain_vec):
    x_f32 = values.astype(jnp.float32)
    scaled = x_f32 * lax.rsqrt(jnp.mean(x_f32 * x_f32, axis=-1, keepdims=True) + NORM_EPS)
    return scaled * (1.0 + gain_vec.astype(jnp.float32))


def rotary(values, positions):
    half_dim = values.shape[-1] // 2
    inv_freq = ROPE_BASE ** (-2.0 * jnp.arange(half_dim, dtype=jnp.float32) / values.shape[-1])
    angles = positions.astype(jnp.float32)[:, None] * inv_freq[None, :]
    angles = angles.reshape((values.shape[0],) + (1,) * (values.ndim - 2) + (half_dim,))
    cos_t = jnp.cos(angles)
    sin_t = jnp.sin(angles)
    x_low = values[..., :half_dim]
    x_high = values[..., half_dim:]
    return jnp.concatenate([x_low * cos_t - x_high * sin_t, x_high * cos_t + x_low * sin_t], axis=-1)


def setup_inputs(seed: int = 0) -> dict:
    keys = jax.random.split(jax.random.key(seed), 20)

    def normal_draw(sub_key, dims, scale_by):
        return (jax.random.normal(sub_key, dims, jnp.float32) * scale_by).astype(jnp.bfloat16)

    int_keys = jax.random.split(keys[19], 4)
    token_ids = jnp.arange(TOKENS)
    seq_lens = jax.random.randint(int_keys[0], (TOKENS,), 1, CTX + 1)
    picked = jax.random.permutation(int_keys[1], TOKENS)
    seq_lens = jnp.where(token_ids == picked[0], CTX, seq_lens)
    seq_lens = jnp.where(token_ids == picked[1], 1, seq_lens).astype(jnp.int32)
    stride = VOCAB // TOKENS
    target = token_ids * stride + jax.random.randint(int_keys[2], (TOKENS,), 0, stride)
    target = jax.random.permutation(int_keys[3], target).astype(jnp.int32)
    d_scale = D ** -0.5
    return {
        'hidden_in': normal_draw(keys[0], (TOKENS, D), 1.0),
        'seq_lens': seq_lens,
        'target': target,
        'g_attn_pre': normal_draw(keys[1], (D,), 0.4),
        'w_q': normal_draw(keys[2], (D, HEADS * HEAD), 4.0 * d_scale),
        'w_k': normal_draw(keys[3], (D, KV_HEADS * HEAD), 4.0 * d_scale),
        'w_v': normal_draw(keys[4], (D, KV_HEADS * HEAD), d_scale),
        'w_o': normal_draw(keys[5], (HEADS * HEAD, D), (HEADS * HEAD) ** -0.5),
        'g_attn_post': normal_draw(keys[6], (D,), 0.4),
        'g_mlp_pre': normal_draw(keys[7], (D,), 0.4),
        'w_gate': normal_draw(keys[8], (D, FF), d_scale),
        'w_up': normal_draw(keys[9], (D, FF), d_scale),
        'w_down': normal_draw(keys[10], (FF, D), FF ** -0.5),
        'g_mlp_post': normal_draw(keys[11], (D,), 0.4),
        'g_final': normal_draw(keys[12], (D,), 0.4),
        'k_cache': normal_draw(keys[13], (TOKENS, CTX, KV_HEADS, HEAD), 4.0),
        'v_cache': normal_draw(keys[14], (TOKENS, CTX, KV_HEADS, HEAD), 1.0),
        'embed_table': normal_draw(keys[15], (VOCAB, D), 25.0 * d_scale),
    }


def reference(hidden_in, seq_lens, target, g_attn_pre, w_q, w_k, w_v, w_o, g_attn_post, g_mlp_pre, w_gate, w_up, w_down, g_mlp_post, g_final, k_cache, v_cache, embed_table):
    group_size = HEADS // KV_HEADS
    score_scale = HEAD ** -0.5
    normed = rms_norm(hidden_in, g_attn_pre).astype(jnp.bfloat16)
    q_rot = rotary(jnp.dot(normed, w_q, preferred_element_type=jnp.float32).reshape(TOKENS, KV_HEADS, group_size, HEAD), seq_lens).astype(jnp.bfloat16)
    k_rot = rotary(jnp.dot(normed, w_k, preferred_element_type=jnp.float32).reshape(TOKENS, KV_HEADS, HEAD), seq_lens).astype(jnp.bfloat16)
    v_new = jnp.dot(normed, w_v, preferred_element_type=jnp.float32).astype(jnp.bfloat16).reshape(TOKENS, KV_HEADS, HEAD)

    def attend(operands):
        q_tok, k_tok, v_tok, keys_tok, vals_tok, len_tok = operands
        q_f32 = q_tok.astype(jnp.float32)
        s_cache = jnp.einsum('kgd,tkd->kgt', q_f32, keys_tok.astype(jnp.float32)) * score_scale
        s_new = jnp.einsum('kgd,kd->kg', q_f32, k_tok.astype(jnp.float32)) * score_scale
        s_cache = ATTN_CAP * jnp.tanh(s_cache / ATTN_CAP)
        s_new = ATTN_CAP * jnp.tanh(s_new / ATTN_CAP)
        s_cache = jnp.where(jnp.arange(CTX) < len_tok, s_cache, -1e30)
        row_max = jnp.maximum(jnp.max(s_cache, axis=-1), s_new)
        p_cache = jnp.exp(s_cache - row_max[..., None])
        p_new = jnp.exp(s_new - row_max)
        denominator = jnp.sum(p_cache, axis=-1) + p_new
        weighted = jnp.einsum('kgt,tkd->kgd', p_cache.astype(jnp.bfloat16).astype(jnp.float32), vals_tok.astype(jnp.float32))
        weighted = weighted + p_new.astype(jnp.bfloat16).astype(jnp.float32)[..., None] * v_tok.astype(jnp.float32)[:, None, :]
        return (weighted / denominator[..., None]).astype(jnp.bfloat16)

    attn_vec = lax.map(attend, (q_rot, k_rot, v_new, k_cache, v_cache, seq_lens))
    attn_out = jnp.dot(attn_vec.reshape(TOKENS, HEADS * HEAD), w_o, preferred_element_type=jnp.float32)
    hidden_mid = (hidden_in.astype(jnp.float32) + rms_norm(attn_out, g_attn_post)).astype(jnp.bfloat16)
    mlp_in = rms_norm(hidden_mid, g_mlp_pre).astype(jnp.bfloat16)
    gate_proj = jnp.dot(mlp_in, w_gate, preferred_element_type=jnp.float32)
    up_proj = jnp.dot(mlp_in, w_up, preferred_element_type=jnp.float32)
    activated = (jax.nn.gelu(gate_proj, approximate=True) * up_proj).astype(jnp.bfloat16)
    mlp_out = jnp.dot(activated, w_down, preferred_element_type=jnp.float32)
    hidden_out = (hidden_mid.astype(jnp.float32) + rms_norm(mlp_out, g_mlp_post)).astype(jnp.bfloat16)
    final_h = rms_norm(hidden_out, g_final).astype(jnp.bfloat16)

    blocks = 16
    block_rows = VOCAB // blocks
    table_blocks = embed_table.reshape(blocks, block_rows, D)
    starts = jnp.arange(blocks) * block_rows

    def block_stats(operands):
        table_block, start_row = operands
        logits = jnp.dot(final_h, table_block.T, preferred_element_type=jnp.float32)
        capped = FINAL_CAP * jnp.tanh(logits / FINAL_CAP)
        block_max = jnp.max(capped, axis=1)
        block_sum = jnp.sum(jnp.exp(capped - block_max[:, None]), axis=1)
        hit_mask = (start_row + jnp.arange(block_rows))[None, :] == target[:, None]
        block_tgt = jnp.sum(jnp.where(hit_mask, capped, 0.0), axis=1)
        return block_max, block_sum, block_tgt

    all_max, all_sum, all_tgt = lax.map(block_stats, (table_blocks, starts))
    glob_max = jnp.max(all_max, axis=0)
    log_norm = glob_max + jnp.log(jnp.sum(all_sum * jnp.exp(all_max - glob_max[None, :]), axis=0))
    logprob = jnp.sum(all_tgt, axis=0) - log_norm
    return logprob, hidden_out
```

```python
import functools

import jax
import jax.numpy as jnp
import numpy as np
from jax import lax
from jax.experimental import pallas as pl
from jax.experimental.pallas import tpu as pltpu
from jax.sharding import PartitionSpec as P

ATTN_CAP = 50.0
FINAL_CAP = 30.0
NORM_EPS = 1e-6
ROPE_BASE = 10000.0
MESH = pl.DeviceIdType.MESH
F32 = jnp.float32
BF16 = jnp.bfloat16


def dot(a, b):
    return jnp.dot(a, b, preferred_element_type=F32)


def dot_nt(a, b):
    return lax.dot_general(a, b, (((1,), (1,)), ((), ())), preferred_element_type=F32)


def rms(values, gain):
    mean_sq = jnp.mean(values * values, axis=-1, keepdims=True)
    return values * lax.rsqrt(mean_sq + NORM_EPS) * (1.0 + gain)


def kernel(NT, NY, NZ, seq, hid, tgt, inv_freq, g_ap, g_ao, g_mp, g_mo, g_fi, wq, wk, wv, wo, wg, wu, wd, kc, vc, emb,
           out_lp, out_y,
           hid_v, wq_v, wk_v, wv_v, kb, vb, wo_v, wg_v, wu_v, wd_v, emb_v,
           p1, q1, h1, a1, act, s2, r2, xs, gs, zb, g_all, h_v, fz, fy, fx, fc,
           lsem, kvsem, ssem, c_rs, x_rs, r_rs, z_rs, a_rs, b_rs, d_rs, fz_rs, fy_rs, fx_rs):
    D = hid.shape[1]
    N = hid.shape[0]
    HD = wk.shape[1]
    FH = wg_v.shape[1]
    L = D // 128
    LP = s2.shape[0] // (2 * NT)
    R = 2 * NT
    DH = D // 2
    CTX = kc.shape[1]
    t = lax.axis_index('t')
    v = lax.axis_index('v')
    c = lax.rem(v, 2)
    y = lax.rem(v // 2, NY)
    z = v // (2 * NY)
    me_r = 2 * t + c

    def dev(tt, zz, yy, cc):
        return {'t': tt, 'v': (zz * NY + yy) * 2 + cc}

    partner = dev(t, z, y, 1 - c)
    x_peers = [(lax.rem(t + k, NT), dev(lax.rem(t + k, NT), z, y, c)) for k in range(1, NT)]
    y_peers = [(lax.rem(y + k, NY), dev(t, z, lax.rem(y + k, NY), c)) for k in range(1, NY)]
    z_peers = [(lax.rem(z + k, NZ), dev(t, lax.rem(z + k, NZ), y, c)) for k in range(1, NZ)]
    r_peers = []
    for k in range(1, R):
        rr = lax.rem(me_r + k, R)
        r_peers.append((rr, dev(rr // 2, z, y, lax.rem(rr, 2))))
    own_a = jnp.where(c == 0, y, t)
    own_b = jnp.where(c == 0, t, y)
    a_peers = []
    b_peers = []
    for k in range(1, NT):
        a_peers.append((lax.rem(own_a + k, NT), dev(lax.rem(t + k * c, NT), z, lax.rem(y + k * (1 - c), NY), c)))
        b_peers.append((lax.rem(own_b + k, NT), dev(lax.rem(t + k * (1 - c), NT), z, lax.rem(y + k * c, NY), c)))

    def token_of(r):
        rx, rc = r // 2, r % 2
        if rc == 0:
            return (rx * NT + y) * NZ + z
        return ((NT + y) * NT + rx) * NZ + z

    tokens = [token_of(r) for r in range(R)]
    chd = pl.ds(pl.multiple_of(c * HD, HD), HD)
    cfh = pl.ds(pl.multiple_of(c * FH, 128), FH)
    loads = {}

    def load(name, src, dst, sem):
        loads[name] = pltpu.make_async_copy(src, dst, sem)
        loads[name].start()

    load('hid', hid, hid_v, lsem.at[0])
    load('wq', wq.at[:, chd], wq_v, lsem.at[1])
    load('wk', wk, wk_v, lsem.at[2])
    load('wv', wv, wv_v, lsem.at[3])
    for r in range(R):
        load('k%d' % r, kc.at[tokens[r]], kb.at[r], kvsem.at[r])
    for r in range(R):
        load('v%d' % r, vc.at[tokens[r]], vb.at[r], kvsem.at[R + r])
    load('wo', wo.at[chd], wo_v, lsem.at[4])
    load('wg', wg.at[:, cfh], wg_v, lsem.at[5])
    load('wu', wu.at[:, cfh], wu_v, lsem.at[6])
    load('wd', wd.at[cfh], wd_v, lsem.at[7])
    load('emb', emb, emb_v, lsem.at[8])

    barrier = pltpu.get_barrier_semaphore()
    greeted = [partner] + [d for _, d in x_peers + y_peers + z_peers]
    for k in range(1, NT):
        greeted.append(dev(lax.rem(t + k, NT), z, y, 1 - c))
    for d in greeted:
        pl.semaphore_signal(barrier, inc=1, device_id=d, device_id_type=MESH)

    sent = []

    def send(src, dst, recv_sem, device):
        copy = pltpu.make_async_remote_copy(
            src_ref=src, dst_ref=dst, send_sem=ssem.at[len(sent)], recv_sem=recv_sem,
            device_id=device, device_id_type=MESH)
        copy.start()
        sent.append(copy)

    def arrived(ref, recv_sem):
        pltpu.make_async_remote_copy(
            src_ref=ref, dst_ref=ref, send_sem=ssem.at[0], recv_sem=recv_sem,
            device_id=partner, device_id_type=MESH).wait_recv()

    s2[...] = jnp.zeros_like(s2)
    xs[...] = jnp.zeros_like(xs)
    gs[...] = jnp.zeros_like(gs)
    g_mo_row = g_mo[...].astype(F32).reshape(1, D)
    for l in range(L):
        gs[pl.ds(l, 1), :] = g_mo_row[:, 128 * l:128 * (l + 1)]

    rr = lax.broadcasted_iota(jnp.int32, (R, 1), 0)
    rx, rc = lax.shift_right_logical(rr, 1), jnp.bitwise_and(rr, 1)
    token_col = jnp.where(rc == 0, (rx * NT + y) * NZ + z, ((NT + y) * NT + rx) * NZ + z)
    pick = jnp.where(lax.broadcasted_iota(jnp.int32, (R, N), 1) == token_col, 1.0, 0.0).astype(BF16)
    pos = jnp.zeros((R, 1), jnp.int32)
    for r in range(R):
        pos = jnp.where(rr == r, seq[tokens[r]], pos)
    angles = pos.astype(F32) * inv_freq[...]
    cos_t = jnp.cos(angles)
    sin_t = jnp.sin(angles)

    def rotary(values):
        low, high = values[:, :HD // 2], values[:, HD // 2:]
        return jnp.concatenate([low * cos_t - high * sin_t, high * cos_t + low * sin_t], axis=-1).astype(BF16)

    loads['hid'].wait()
    x = dot(pick, hid_v[...])
    normed = rms(x, g_ap[...].astype(F32).reshape(1, D)).astype(BF16)
    loads['wq'].wait()
    q_rot = rotary(dot(normed, wq_v[...]))
    loads['wk'].wait()
    k_rot = rotary(dot(normed, wk_v[...]))
    loads['wv'].wait()
    v_new = dot(normed, wv_v[...]).astype(BF16)
    scale = HD ** -0.5
    s_cache = jnp.zeros((R, CTX), F32)
    for r in range(R):
        loads['k%d' % r].wait()
        s_cache = jnp.where(rr == r, dot_nt(q_rot, kb[r]), s_cache)
    s_new = jnp.sum(q_rot.astype(F32) * k_rot.astype(F32), axis=-1, keepdims=True) * scale
    s_cache = ATTN_CAP * jnp.tanh(s_cache * scale / ATTN_CAP)
    s_new = ATTN_CAP * jnp.tanh(s_new / ATTN_CAP)
    valid = lax.broadcasted_iota(jnp.int32, (R, CTX), 1) < pos
    s_cache = jnp.where(valid, s_cache, -1e30)
    row_max = jnp.maximum(jnp.max(s_cache, axis=-1, keepdims=True), s_new)
    p_cache = jnp.exp(s_cache - row_max)
    p_new = jnp.exp(s_new - row_max)
    denominator = jnp.sum(p_cache, axis=-1, keepdims=True) + p_new
    p_bf = p_cache.astype(BF16)
    weighted = jnp.zeros((R, HD), F32)
    for r in range(R):
        loads['v%d' % r].wait()
        weighted = jnp.where(rr == r, dot(p_bf, vb[r]), weighted)
    weighted = weighted + p_new.astype(BF16).astype(F32) * v_new.astype(F32)
    attn_vec = (weighted / denominator).astype(BF16)
    loads['wo'].wait()
    attn_part = dot(attn_vec, wo_v[...])
    p1[0] = attn_part[:, :DH]
    p1[1] = attn_part[:, DH:]

    pl.semaphore_wait(barrier, len(greeted))
    send(p1.at[1 - c], q1, c_rs.at[0], partner)
    arrived(q1, c_rs.at[0])
    h1[t] = p1[c] + q1[...]
    for _, d in x_peers:
        send(h1.at[t], h1.at[t], x_rs.at[t], d)
    for k, _ in x_peers:
        arrived(h1.at[k], x_rs.at[k])
    half = h1[0]
    for k in range(1, NT):
        half = half + h1[k]
    a1[c] = half
    send(a1.at[c], a1.at[c], c_rs.at[1], partner)
    arrived(a1.at[1 - c], c_rs.at[1])
    attn_out = jnp.concatenate([a1[0], a1[1]], axis=-1)
    mid = (x + rms(attn_out, g_ao[...].astype(F32).reshape(1, D))).astype(BF16).astype(F32)
    for l in range(L):
        xs[pl.ds(l, R, stride=LP), :] = mid[:, 128 * l:128 * (l + 1)]
    mlp_in = rms(mid, g_mp[...].astype(F32).reshape(1, D)).astype(BF16)

    loads['wg'].wait()
    loads['wu'].wait()
    width = 384 if FH % 384 == 0 else 128
    for j in range(FH // width):
        cols = pl.ds(j * width, width)
        gate = dot(mlp_in, wg_v[:, cols])
        up = dot(mlp_in, wu_v[:, cols])
        act[:, cols] = (jax.nn.gelu(gate, approximate=True) * up).astype(BF16)
    loads['wd'].wait()
    width = 768 if D % 768 == 0 else 128
    for j in range(D // width):
        part = dot(act[...], wd_v[:, pl.ds(j * width, width)])
        for i in range(width // 128):
            s2[pl.ds(j * (width // 128) + i, R, stride=LP), :] = part[:, 128 * i:128 * (i + 1)]

    def slot(k):
        return pl.ds(pl.multiple_of(k * LP, 8), LP)

    for k, d in r_peers:
        send(s2.at[slot(k)], r2.at[slot(me_r)], r_rs.at[me_r], d)
    r2[slot(me_r), :] = s2[slot(me_r), :]
    for k, _ in r_peers:
        arrived(r2.at[slot(k)], r_rs.at[k])
    row = r2[pl.ds(0, LP), :]
    for k in range(1, R):
        row = row + r2[pl.ds(k * LP, LP), :]
    mean_sq = jnp.sum(jnp.sum(row * row, axis=0, keepdims=True), axis=1, keepdims=True) * (1.0 / D)
    row = row * lax.rsqrt(mean_sq + NORM_EPS) * (1.0 + gs[...])
    zb[slot(z), :] = (xs[slot(me_r), :] + row).astype(BF16).astype(F32)

    for _, d in z_peers:
        send(zb.at[slot(z)], zb.at[slot(z)], z_rs.at[z], d)
    for k, _ in z_peers:
        arrived(zb.at[slot(k)], z_rs.at[k])
    first = c * NT + own_b
    mine = first * NT + own_a
    for l in range(L):
        g_all[mine, :, 128 * l:128 * (l + 1)] = zb[pl.ds(l, NZ, stride=LP), :]
    for _, d in a_peers:
        send(g_all.at[mine], g_all.at[mine], a_rs.at[own_a], d)
    for k, _ in a_peers:
        arrived(g_all.at[first * NT + k], a_rs.at[k])
    whole = pl.ds(first * NT, NT)
    for _, d in b_peers:
        send(g_all.at[whole], g_all.at[whole], b_rs.at[own_b], d)
    send(g_all.at[whole], g_all.at[whole], d_rs.at[own_b], partner)
    for k, _ in b_peers:
        piece = pl.ds((c * NT + k) * NT, NT)
        arrived(g_all.at[piece], b_rs.at[k])
        send(g_all.at[piece], g_all.at[piece], d_rs.at[k], partner)

    g_fi_row = g_fi[...].astype(F32).reshape(1, D)
    step = min(16 // NZ, NT * NT)
    width = step * NZ

    def final_norm(core):
        def body(i, carry):
            blk = core * (NT * NT) + i * step
            ys = g_all[pl.ds(blk, step)].reshape(width, D)
            rows = pl.ds(pl.multiple_of(blk * NZ, width), width)
            out_y[rows, :] = ys.astype(BF16)
            h_v[rows, :] = rms(ys, g_fi_row).astype(BF16)
            return carry
        lax.fori_loop(0, NT * NT // step, body, 0)

    final_norm(c)
    for k in range(NT):
        arrived(g_all.at[pl.ds(((1 - c) * NT + k) * NT, NT)], d_rs.at[k])
    final_norm(1 - c)

    loads['emb'].wait()
    VL = emb.shape[0]
    rows_at = 0
    total = jnp.zeros((1, N), F32)
    hit = jnp.zeros((1, N), F32)
    target = tgt[...].reshape(1, N) - (v * NT + t) * VL
    while rows_at < VL:
        size = min(256, VL - rows_at)
        logits = dot_nt(emb_v[pl.ds(rows_at, size), :], h_v[...])
        capped = FINAL_CAP * jnp.tanh(logits / FINAL_CAP)
        total = total + jnp.sum(jnp.exp(capped), axis=0, keepdims=True)
        ids = rows_at + lax.broadcasted_iota(jnp.int32, (size, N), 0)
        hit = hit + jnp.sum(jnp.where(ids == target, capped, 0.0), axis=0, keepdims=True)
        rows_at += size
    stats = jnp.concatenate([total, hit], axis=0)

    for buf, sems, me, peers, count in (
        (fz, fz_rs, z, z_peers, NZ), (fy, fy_rs, y, y_peers, NY), (fx, fx_rs, t, x_peers, NT),
        (fc, None, c, [(1 - c, partner)], 2)):
        buf[me] = stats
        for k, d in peers:
            send(buf.at[me], buf.at[me], c_rs.at[2] if sems is None else sems.at[me], d)
        for k, d in peers:
            arrived(buf.at[k], c_rs.at[2] if sems is None else sems.at[k])
        stats = buf[0]
        for k in range(1, count):
            stats = stats + buf[k]
    out_lp[...] = stats[1:2, :] - jnp.log(stats[0:1, :])
    for copy in sent:
        copy.wait_send()


def solution(mesh):
    NT = mesh.shape['t']
    V = mesh.shape['v']
    NY = NT
    NZ = V // (2 * NY)
    in_specs = (P(), P(), P(), P(), P(None, 't'), P(None, 't'), P(None, 't'), P('t', None), P(), P(), P(None, 't'), P(None, 't'), P('t', None), P(), P(), P(None, None, 't', None), P(None, None, 't', None), P(('v', 't'), None))

    def local_step(hidden_in, seq_lens, target, g_attn_pre, w_q, w_k, w_v, w_o, g_attn_post, g_mlp_pre, w_gate, w_up, w_down, g_mlp_post, g_final, k_cache, v_cache, embed_table):
        N, D = hidden_in.shape
        CTX, _, HD = k_cache.shape[1:]
        FH = w_gate.shape[1] // 2
        VL = embed_table.shape[0]
        R = 2 * NT
        LP = (D // 128 + 7) // 8 * 8
        inv_freq = (ROPE_BASE ** (-2.0 * np.arange(HD // 2, dtype=np.float32) / HD)).astype(np.float32).reshape(1, HD // 2)
        any_spec = pl.BlockSpec(memory_space=pl.ANY)
        vmem = pl.BlockSpec(memory_space=pltpu.VMEM)
        smem = pl.BlockSpec(memory_space=pltpu.SMEM)
        sends = 3 + 3 * (NT - 1) + (R - 1) + (NZ - 1) + NT + (NZ - 1) + (NY - 1) + (NT - 1) + 1
        dma = pltpu.SemaphoreType.DMA
        lp, hidden_out = pl.pallas_call(
            functools.partial(kernel, NT, NY, NZ),
            name='decode_step',
            out_shape=(jax.ShapeDtypeStruct((1, N), F32), jax.ShapeDtypeStruct((N, D), BF16)),
            in_specs=[smem, any_spec] + [vmem] * 7 + [any_spec] * 10,
            out_specs=(vmem, vmem),
            scratch_shapes=[
                pltpu.VMEM((N, D), BF16), pltpu.VMEM((D, HD), BF16), pltpu.VMEM((D, HD), BF16), pltpu.VMEM((D, HD), BF16),
                pltpu.VMEM((R, CTX, HD), BF16), pltpu.VMEM((R, CTX, HD), BF16), pltpu.VMEM((HD, D), BF16),
                pltpu.VMEM((D, FH), BF16), pltpu.VMEM((D, FH), BF16), pltpu.VMEM((FH, D), BF16), pltpu.VMEM((VL, D), BF16),
                pltpu.VMEM((2, R, D // 2), F32), pltpu.VMEM((R, D // 2), F32), pltpu.VMEM((NT, R, D // 2), F32),
                pltpu.VMEM((2, R, D // 2), F32), pltpu.VMEM((R, FH), BF16),
                pltpu.VMEM((R * LP, 128), F32), pltpu.VMEM((R * LP, 128), F32), pltpu.VMEM((R * LP, 128), F32),
                pltpu.VMEM((LP, 128), F32), pltpu.VMEM((NZ * LP, 128), F32),
                pltpu.VMEM((2 * NT * NT, NZ, D), F32), pltpu.VMEM((N, D), BF16),
                pltpu.VMEM((NZ, 2, N), F32), pltpu.VMEM((NY, 2, N), F32), pltpu.VMEM((NT, 2, N), F32), pltpu.VMEM((2, 2, N), F32),
                dma((9,)), dma((2 * R,)), dma((sends,)), dma((3,)), dma((NT,)), dma((R,)), dma((NZ,)), dma((NT,)), dma((NT,)),
                dma((NT,)), dma((NZ,)), dma((NY,)), dma((NT,)),
            ],
            compiler_params=pltpu.CompilerParams(
                collective_id=0, has_side_effects=True, vmem_limit_bytes=60 * 1024 * 1024),
        )(seq_lens, hidden_in, target, inv_freq, g_attn_pre, g_attn_post, g_mlp_pre, g_mlp_post, g_final,
          w_q, w_k, w_v, w_o, w_gate, w_up, w_down,
          k_cache.reshape(N, CTX, HD), v_cache.reshape(N, CTX, HD), embed_table)
        return lp.reshape(N), hidden_out

    return jax.shard_map(local_step, mesh=mesh, in_specs=in_specs, out_specs=(P(), P()), check_vma=False)
```

```python
import functools

import jax
import jax.numpy as jnp
import numpy as np
from jax import lax
from jax.experimental import pallas as pl
from jax.experimental.pallas import tpu as pltpu
from jax.sharding import PartitionSpec as P

ATTN_CAP = 50.0
FINAL_CAP = 30.0
NORM_EPS = 1e-6
ROPE_BASE = 10000.0
MESH = pl.DeviceIdType.MESH
F32 = jnp.float32
BF16 = jnp.bfloat16
VMEM_LIMIT = 60 * 1024 * 1024


def dot(a, b):
    return jnp.dot(a, b, preferred_element_type=F32)


def dot_nt(a, b):
    return lax.dot_general(a, b, (((1,), (1,)), ((), ())), preferred_element_type=F32)


def rms(values, gain):
    mean_sq = jnp.mean(values * values, axis=-1, keepdims=True)
    return values * lax.rsqrt(mean_sq + NORM_EPS) * (1.0 + gain)


def kernel(NT, NY, NZ, seq_h, hid, tgt_h, freq_h, ap_h, ao_h, mp_h, mo_h, fi_h, wq, wk, wv, wo, wg, wu, wd, kc, vc, emb,
           out_lp, out_y,
           seq, tgt, inv_freq, g_ap, g_ao, g_mp, g_mo, g_fi, y_v, hid_v, wq_v, wk_v, wv_v, kb, vb, wo_v, wg_v, wu_v, wd_v, emb_v,
           act, s1, s2, r1, r2, m1, xs, gs, gt, h_v, fz, fx,
           lsem, ssem, r_rs, z_rs, a_rs, b_rs, d_rs, f_rs):
    N, D = hid.shape
    HD = wk.shape[1]
    FH = wg_v.shape[1]
    CTX = kc.shape[1]
    VL = emb.shape[0]
    L = D // 128
    R = 2 * NT
    LP = s1.shape[0] // R
    PZ = NZ // 2
    t = lax.axis_index('t')
    v = lax.axis_index('v')
    c = lax.rem(v, 2)
    y = lax.rem(v // 2, NY)
    z = v // (2 * NY)
    me_r = 2 * t + c

    def dev(tt, zz, yy, cc):
        return {'t': tt, 'v': (zz * NY + yy) * 2 + cc}

    partner = dev(t, z, y, 1 - c)
    near_first = sorted(range(1, NZ), key=lambda k: min(k, NZ - k))
    ring = [k for k in (1, NT - 1, 2) if 0 < k < NT]
    ring = sorted(set(ring), key=ring.index)
    z_peers = [(lax.rem(z + k, NZ), dev(t, lax.rem(z + k, NZ), y, c)) for k in near_first]
    r_peers = []
    for k in range(1, R):
        rr = lax.rem(me_r + k, R)
        r_peers.append((rr, dev(rr // 2, z, y, lax.rem(rr, 2))))
    own_a = jnp.where(c == 0, y, t)
    own_b = jnp.where(c == 0, t, y)
    a_peers = []
    b_peers = []
    for k in ring:
        a_peers.append((lax.rem(own_a + k, NT), dev(lax.rem(t + k * c, NT), z, lax.rem(y + k * (1 - c), NY), c)))
        b_peers.append((lax.rem(own_b + k, NT), dev(lax.rem(t + k * (1 - c), NT), z, lax.rem(y + k * c, NY), c)))
    zc_peers = []
    for dz in [0] + near_first:
        for dc in (0, 1):
            if dz or dc:
                zz, cc = lax.rem(z + dz, NZ), (c if dc == 0 else 1 - c)
                zc_peers.append((zz * 2 + cc, dev(t, zz, y, cc)))
    xy_peers = []
    for dx in range(NT):
        for dy in range(NY):
            if dx or dy:
                xx, yy = lax.rem(t + dx, NT), lax.rem(y + dy, NY)
                xy_peers.append((xx * NY + yy, dev(xx, z, yy, c)))

    def token_of(r):
        rx, rc = r // 2, r % 2
        if rc == 0:
            return (rx * NT + y) * NZ + z
        return ((NT + y) * NT + rx) * NZ + z

    tokens = [token_of(r) for r in range(R)]
    chd = pl.ds(pl.multiple_of(c * HD, HD), HD)
    cfh = pl.ds(pl.multiple_of(c * FH, 128), FH)
    loads = {}

    def load(name, src, dst, sem):
        loads[name] = pltpu.make_async_copy(src, dst, sem)
        loads[name].start()

    load('seq', seq_h, seq, lsem.at[11])
    load('freq', freq_h, inv_freq, lsem.at[12])
    load('ap', ap_h, g_ap, lsem.at[13])
    load('hid', hid, hid_v, lsem.at[0])
    load('wq', wq.at[:, chd], wq_v, lsem.at[1])
    load('wk', wk, wk_v, lsem.at[2])
    load('wv', wv, wv_v, lsem.at[3])
    for r in range(R):
        load('k%d' % r, kc.at[tokens[r]], kb.at[r], lsem.at[9])
    for r in range(R):
        load('v%d' % r, vc.at[tokens[r]], vb.at[r], lsem.at[10])
    for i, (src, dst) in enumerate(((tgt_h, tgt), (ao_h, g_ao), (mp_h, g_mp), (mo_h, g_mo), (fi_h, g_fi))):
        load('small%d' % i, src, dst, lsem.at[14 + i])
    load('wo', wo.at[chd], wo_v, lsem.at[4])
    load('wg', wg.at[:, cfh], wg_v, lsem.at[5])
    load('wu', wu.at[:, cfh], wu_v, lsem.at[6])
    load('wd', wd.at[cfh], wd_v, lsem.at[7])
    load('emb', emb, emb_v, lsem.at[8])

    barrier = pltpu.get_barrier_semaphore()
    greeted = [d for _, d in zc_peers + xy_peers]
    for k in range(1, NT):
        greeted.append(dev(lax.rem(t + k, NT), z, y, 1 - c))
    for d in greeted:
        pl.semaphore_signal(barrier, inc=1, device_id=d, device_id_type=MESH)

    def send(src, dst, lane, recv_sem, device):
        pltpu.make_async_remote_copy(
            src_ref=src, dst_ref=dst, send_sem=ssem.at[lane], recv_sem=recv_sem,
            device_id=device, device_id_type=MESH).start()

    def all_sent(ref, lane):
        pltpu.make_async_remote_copy(
            src_ref=ref, dst_ref=ref, send_sem=ssem.at[lane], recv_sem=z_rs.at[0],
            device_id=partner, device_id_type=MESH).wait_send()

    def arrived(ref, recv_sem):
        pltpu.make_async_remote_copy(
            src_ref=ref, dst_ref=ref, send_sem=ssem.at[0], recv_sem=recv_sem,
            device_id=partner, device_id_type=MESH).wait_recv()

    for buf in (s1, s2, xs, gs):
        buf[...] = jnp.zeros_like(buf)
    def slot(k):
        return pl.ds(pl.multiple_of(k * LP, 8), LP)

    def to_rows(buf, values, at):
        for i in range(values.shape[1] // 128):
            buf[pl.ds(at + i, R, stride=LP), :] = values[:, 128 * i:128 * (i + 1)]

    others = pl.ds(0, (R - 1) * LP)

    def reduce_rows(src, dst, lane):
        for k, d in r_peers:
            send(src.at[slot(k)], dst.at[slot(me_r)], lane, r_rs.at[lane], d)
        dst[slot(me_r), :] = src[slot(me_r), :]
        arrived(dst.at[others], r_rs.at[lane])
        row = dst[pl.ds(0, LP), :]
        for k in range(1, R):
            row = row + dst[pl.ds(k * LP, LP), :]
        return row

    def rms_row(row, i):
        mean_sq = jnp.sum(jnp.sum(row * row, axis=0, keepdims=True), axis=1, keepdims=True) * (1.0 / D)
        return row * lax.rsqrt(mean_sq + NORM_EPS) * (1.0 + gs[pl.ds(i * LP, LP), :])

    rr = lax.broadcasted_iota(jnp.int32, (R, 1), 0)
    rx, rc = lax.shift_right_logical(rr, 1), jnp.bitwise_and(rr, 1)
    token_col = jnp.where(rc == 0, (rx * NT + y) * NZ + z, ((NT + y) * NT + rx) * NZ + z)
    pick = jnp.where(lax.broadcasted_iota(jnp.int32, (R, N), 1) == token_col, 1.0, 0.0).astype(BF16)
    loads['seq'].wait()
    loads['freq'].wait()
    loads['ap'].wait()
    pos = jnp.zeros((R, 1), jnp.int32)
    for r in range(R):
        pos = jnp.where(rr == r, seq[tokens[r]], pos)
    angles = pos.astype(F32) * inv_freq[...]
    cos_t = jnp.cos(angles)
    sin_t = jnp.sin(angles)

    def rotary(values):
        low, high = values[:, :HD // 2], values[:, HD // 2:]
        return jnp.concatenate([low * cos_t - high * sin_t, high * cos_t + low * sin_t], axis=-1).astype(BF16)

    loads['hid'].wait()
    x = dot(pick, hid_v[...])
    normed = rms(x, g_ap[...].astype(F32).reshape(1, D)).astype(BF16)
    to_rows(xs, x, 0)
    for name in ('wq', 'wk', 'wv'):
        loads[name].wait()
    q_rot = rotary(dot(normed, wq_v[...]))
    k_rot = rotary(dot(normed, wk_v[...]))
    v_new = dot(normed, wv_v[...]).astype(BF16)
    scale = HD ** -0.5
    pltpu.make_async_copy(kb, kb, lsem.at[9]).wait()
    scores = [dot_nt(q_rot, kb[r]) for r in range(R)]
    s_cache = scores[0]
    for r in range(1, R):
        s_cache = jnp.where(rr == r, scores[r], s_cache)
    s_new = jnp.sum(q_rot.astype(F32) * k_rot.astype(F32), axis=-1, keepdims=True) * scale
    s_cache = ATTN_CAP * jnp.tanh(s_cache * scale / ATTN_CAP)
    s_new = ATTN_CAP * jnp.tanh(s_new / ATTN_CAP)
    valid = lax.broadcasted_iota(jnp.int32, (R, CTX), 1) < pos
    s_cache = jnp.where(valid, s_cache, -1e30)
    row_max = jnp.maximum(jnp.max(s_cache, axis=-1, keepdims=True), s_new)
    p_cache = jnp.exp(s_cache - row_max)
    p_new = jnp.exp(s_new - row_max)
    denominator = jnp.sum(p_cache, axis=-1, keepdims=True) + p_new
    p_bf = p_cache.astype(BF16)
    pltpu.make_async_copy(vb, vb, lsem.at[10]).wait()
    parts = [dot(p_bf, vb[r]) for r in range(R)]
    weighted = parts[0]
    for r in range(1, R):
        weighted = jnp.where(rr == r, parts[r], weighted)
    weighted = weighted + p_new.astype(BF16).astype(F32) * v_new.astype(F32)
    attn_vec = (weighted / denominator).astype(BF16)
    loads['wo'].wait()
    to_rows(s1, dot(attn_vec, wo_v[...]), 0)
    for i in range(5):
        loads['small%d' % i].wait()
    for i, gain in enumerate((g_ao, g_mo)):
        gain_row = gain[...].astype(F32).reshape(1, D)
        for l in range(L):
            gs[pl.ds(i * LP + l, 1), :] = gain_row[:, 128 * l:128 * (l + 1)]

    pl.semaphore_wait(barrier, len(greeted))
    row = reduce_rows(s1, r1, 0)
    mid_row = (xs[slot(me_r), :] + rms_row(row, 0)).astype(BF16).astype(F32)
    m1[slot(me_r), :] = mid_row
    for _, d in r_peers:
        send(m1.at[slot(me_r)], m1.at[slot(me_r)], 1, r_rs.at[1], d)
    arrived(m1.at[others], r_rs.at[1])
    mid = jnp.concatenate([m1[pl.ds(l, R, stride=LP), :] for l in range(L)], axis=-1)
    mlp_in = rms(mid, g_mp[...].astype(F32).reshape(1, D)).astype(BF16)

    loads['wg'].wait()
    loads['wu'].wait()
    width = 384 if FH % 384 == 0 else 128
    for j in range(FH // width):
        cols = pl.ds(j * width, width)
        gate = dot(mlp_in, wg_v[:, cols])
        up = dot(mlp_in, wu_v[:, cols])
        act[:, cols] = (jax.nn.gelu(gate, approximate=True) * up).astype(BF16)
    loads['wd'].wait()
    width = 768 if D % 768 == 0 else 128
    for j in range(D // width):
        to_rows(s2, dot(act[...], wd_v[:, pl.ds(j * width, width)]), j * (width // 128))
    row = reduce_rows(s2, r2, 2)
    y_row = (m1[slot(me_r), :] + rms_row(row, 1)).astype(BF16).astype(F32)

    def pair(core, b, a, q):
        return pl.ds((((core * NT + b) * NT + a) * NZ + 2 * q) * L, 2 * L)

    def single(zz):
        return pl.ds((((c * NT + own_b) * NT + own_a) * NZ + zz) * L, L)

    me_at = (((c * NT + own_b) * NT + own_a) * NZ + z) * L
    for l in range(L):
        gt[me_at + l] = y_row[l:l + 1, :]
    my_q = z // 2
    for _, d in z_peers:
        send(gt.at[single(z)], gt.at[single(z)], 3, z_rs.at[my_q], d)

    def rows_of(count):
        return gt.at[pl.ds(0, count * L)]

    def to_b_and_core(a, q, late):
        here = gt.at[pair(c, own_b, a, q)]
        for _, d in b_peers:
            send(here, here, 5, b_rs.at[(own_b * PZ + q) * 2 + late], d)
        send(here, here, 6, d_rs.at[own_b], partner)

    def own_pair(dq):
        q = lax.rem(my_q + dq, PZ)
        arrived(rows_of(1 if dq == 0 else 2), z_rs.at[q])
        here = gt.at[pair(c, own_b, own_a, q)]
        for _, d in a_peers:
            send(here, here, 4, a_rs.at[q], d)
        to_b_and_core(own_a, q, 0)

    def first_axis(dq):
        q = lax.rem(my_q + dq, PZ)
        arrived(rows_of(2 * (NT - 1)), a_rs.at[q])
        for a, _ in a_peers:
            to_b_and_core(a, q, 1)

    if PZ == 4:
        own_pair(0)
        own_pair(1)
        own_pair(3)
        first_axis(0)
        own_pair(2)
        first_axis(1)
        first_axis(3)
        first_axis(2)
    else:
        for dq in range(PZ):
            own_pair(dq)
        for dq in range(PZ):
            first_axis(dq)
    order = [0, 1, 3, 2] if PZ == 4 else list(range(PZ))

    g_fi_row = 1.0 + g_fi[...].astype(F32).reshape(1, D)
    unit = 16 if NT * NZ % 16 == 0 else NT * NZ

    def final_norm(core, b):
        def body(i, carry):
            first = (core * NT + b) * (NT * NZ) + i * unit
            tiles = []
            for l in range(L):
                tiles.append(jnp.concatenate(
                    [gt[pl.ds((first + j) * L + l, NZ, stride=L), 0, :] for j in range(0, unit, NZ)], axis=0))
            square = tiles[0] * tiles[0]
            for l in range(1, L):
                square = square + tiles[l] * tiles[l]
            inv = lax.rsqrt(jnp.sum(square, axis=-1, keepdims=True) * (1.0 / D) + NORM_EPS)
            rows = pl.ds(pl.multiple_of(first, unit), unit)
            for l in range(L):
                cols = slice(128 * l, 128 * (l + 1))
                y_v[rows, cols] = tiles[l].astype(BF16)
                h_v[rows, cols] = (tiles[l] * inv * g_fi_row[:, cols]).astype(BF16)
            return carry
        lax.fori_loop(0, NT * NZ // unit, body, 0)

    final_norm(c, own_b)
    for i, (b, _) in enumerate(b_peers):
        for late, lanes in ((0, [own_a]), (1, [a for a, _ in a_peers])):
            for dq in order:
                q = lax.rem(my_q + dq, PZ)
                arrived(rows_of(2 * len(lanes)), b_rs.at[(b * PZ + q) * 2 + late])
                for a in lanes:
                    piece = gt.at[pair(c, b, a, q)]
                    send(piece, piece, 6, d_rs.at[b], partner)
        if i + 1 < len(b_peers):
            final_norm(c, b)
    final_norm(c, b_peers[-1][0])
    for k in [0] + ring:
        b = lax.rem(own_a + k, NT)
        arrived(rows_of(NT * NZ), d_rs.at[b])
        final_norm(1 - c, b)

    load('y', y_v, out_y, lsem.at[19])

    loads['emb'].wait()
    rows_at = 0
    total = jnp.zeros((1, N), F32)
    hit = jnp.zeros((1, N), F32)
    target = tgt[...].reshape(1, N) - (v * NT + t) * VL
    while rows_at < VL:
        size = min(256, VL - rows_at)
        logits = dot_nt(emb_v[pl.ds(rows_at, size), :], h_v[...])
        capped = FINAL_CAP * jnp.tanh(logits * (1.0 / FINAL_CAP))
        total = total + jnp.sum(jnp.exp(capped), axis=0, keepdims=True)
        ids = rows_at + lax.broadcasted_iota(jnp.int32, (size, N), 0)
        hit = hit + jnp.sum(jnp.where(ids == target, capped, 0.0), axis=0, keepdims=True)
        rows_at += size
    stats = jnp.concatenate([total, hit], axis=0)

    for i, (buf, me, peers) in enumerate(((fz, z * 2 + c, zc_peers), (fx, t * NY + y, xy_peers))):
        buf[me] = stats
        for _, d in peers:
            send(buf.at[me], buf.at[me], 7 + i, f_rs.at[i], d)
        arrived(buf.at[pl.ds(0, len(peers))], f_rs.at[i])
        stats = buf[0]
        for k in range(1, buf.shape[0]):
            stats = stats + buf[k]
    out_lp[...] = stats[1:2, :] - jnp.log(stats[0:1, :])
    loads['y'].wait()
    for lane, ref in enumerate((
            s1.at[others], m1.at[others], s2.at[others], rows_of(NZ - 1), rows_of(PZ * 2 * (NT - 1)),
            rows_of(NT * PZ * 2 * (NT - 1)), rows_of(NT * NT * NZ), fz.at[pl.ds(0, len(zc_peers))],
            fx.at[pl.ds(0, len(xy_peers))])):
        all_sent(ref, lane)


def hand_on(parts, lp_in, y_in, lp_out, y_out, lp_v, y_v, sems):
    rows = y_v.shape[1]
    first = pltpu.make_async_copy(lp_in, lp_v, sems.at[0])
    first.start()
    into = [pltpu.make_async_copy(y_in.at[pl.ds(i * rows, rows)], y_v.at[i], sems.at[1 + i]) for i in range(parts)]
    for copy in into:
        copy.start()
    first.wait()
    out = [pltpu.make_async_copy(lp_v, lp_out, sems.at[1 + parts])]
    out[0].start()
    for i in range(parts):
        into[i].wait()
        out.append(pltpu.make_async_copy(y_v.at[i], y_out.at[pl.ds(i * rows, rows)], sems.at[2 + parts + i]))
        out[-1].start()
    for copy in out:
        copy.wait()


def solution(mesh):
    NT = mesh.shape['t']
    V = mesh.shape['v']
    NY = NT
    NZ = V // (2 * NY)
    in_specs = (P(), P(), P(), P(), P(None, 't'), P(None, 't'), P(None, 't'), P('t', None), P(), P(), P(None, 't'), P(None, 't'), P('t', None), P(), P(), P(None, None, 't', None), P(None, None, 't', None), P(('v', 't'), None))

    def local_step(hidden_in, seq_lens, target, g_attn_pre, w_q, w_k, w_v, w_o, g_attn_post, g_mlp_pre, w_gate, w_up, w_down, g_mlp_post, g_final, k_cache, v_cache, embed_table):
        N, D = hidden_in.shape
        CTX, _, HD = k_cache.shape[1:]
        FH = w_gate.shape[1] // 2
        VL = embed_table.shape[0]
        R = 2 * NT
        LP = (D // 128 + 7) // 8 * 8
        inv_freq = (ROPE_BASE ** (-2.0 * np.arange(HD // 2, dtype=np.float32) / HD)).astype(np.float32).reshape(1, HD // 2)
        vmem = pl.BlockSpec(memory_space=pltpu.VMEM)
        PZ = NZ // 2
        dma = pltpu.SemaphoreType.DMA
        rows = pltpu.VMEM((R * LP, 128), F32)
        lp, hidden_out = pl.pallas_call(
            functools.partial(kernel, NT, NY, NZ),
            name='decode_step',
            out_shape=(jax.ShapeDtypeStruct((1, N), F32), jax.ShapeDtypeStruct((N, D), BF16)),
            in_specs=[pl.BlockSpec(memory_space=pltpu.HBM)] * 19,
            out_specs=(vmem, pl.BlockSpec(memory_space=pltpu.HBM)),
            scratch_shapes=[
                pltpu.SMEM((N,), jnp.int32), pltpu.VMEM((N,), jnp.int32), pltpu.VMEM((1, HD // 2), F32)]
            + [pltpu.VMEM((D,), BF16)] * 5 + [
                pltpu.VMEM((N, D), BF16), pltpu.VMEM((N, D), BF16), pltpu.VMEM((D, HD), BF16), pltpu.VMEM((D, HD), BF16), pltpu.VMEM((D, HD), BF16),
                pltpu.VMEM((R, CTX, HD), BF16), pltpu.VMEM((R, CTX, HD), BF16), pltpu.VMEM((HD, D), BF16),
                pltpu.VMEM((D, FH), BF16), pltpu.VMEM((D, FH), BF16), pltpu.VMEM((FH, D), BF16), pltpu.VMEM((VL, D), BF16),
                pltpu.VMEM((R, FH), BF16), rows, rows, rows, rows, rows, rows, pltpu.VMEM((2 * LP, 128), F32),
                pltpu.VMEM((N * (D // 128), 1, 128), F32), pltpu.VMEM((N, D), BF16),
                pltpu.VMEM((2 * NZ, 2, N), F32), pltpu.VMEM((NT * NY, 2, N), F32),
                dma((20,)), dma((9,)), dma((3,)), dma((PZ,)), dma((PZ,)), dma((NT * PZ * 2,)), dma((NT,)), dma((2,)),
            ],
            compiler_params=pltpu.CompilerParams(
                collective_id=0, has_side_effects=True, vmem_limit_bytes=VMEM_LIMIT),
        )(seq_lens, hidden_in, target, inv_freq, g_attn_pre, g_attn_post, g_mlp_pre, g_mlp_post, g_final,
          w_q, w_k, w_v, w_o, w_gate, w_up, w_down,
          k_cache.reshape(N, CTX, HD), v_cache.reshape(N, CTX, HD), embed_table)
        parts = 4 if N % 64 == 0 else 1
        hbm = pl.BlockSpec(memory_space=pltpu.HBM)
        lp, hidden_out = pl.pallas_call(
            functools.partial(hand_on, parts),
            name='hand_on',
            out_shape=(jax.ShapeDtypeStruct((1, N), F32), jax.ShapeDtypeStruct((N, D), BF16)),
            in_specs=[hbm, hbm],
            out_specs=(hbm, hbm),
            scratch_shapes=[pltpu.VMEM((1, N), F32), pltpu.VMEM((parts, N // parts, D), BF16), dma((2 + 2 * parts,))],
            compiler_params=pltpu.CompilerParams(vmem_limit_bytes=VMEM_LIMIT),
        )(lp, hidden_out)
        return lp.reshape(N), hidden_out

    return jax.shard_map(local_step, mesh=mesh, in_specs=in_specs, out_specs=(P(), P()), check_vma=False)
```

```python
import functools

import jax
import jax.numpy as jnp
import numpy as np
from jax import lax
from jax.experimental import pallas as pl
from jax.experimental.pallas import tpu as pltpu
from jax.sharding import PartitionSpec as P

ATTN_CAP = 50.0
FINAL_CAP = 30.0
NORM_EPS = 1e-6
ROPE_BASE = 10000.0
MESH = pl.DeviceIdType.MESH
F32 = jnp.float32
BF16 = jnp.bfloat16
VMEM_LIMIT = 60 * 1024 * 1024


def dot(a, b):
    return jnp.dot(a, b, preferred_element_type=F32)


def dot_nt(a, b):
    return lax.dot_general(a, b, (((1,), (1,)), ((), ())), preferred_element_type=F32)


def rms(values, gain):
    mean_sq = jnp.mean(values * values, axis=-1, keepdims=True)
    return values * lax.rsqrt(mean_sq + NORM_EPS) * (1.0 + gain)


def kernel(NT, NY, NZ, seq_h, hid, tgt_h, freq_h, ap_h, ao_h, mp_h, mo_h, fi_h, wq, wk, wv, wo, wg, wu, wd, kc, vc, emb,
           out_lp, out_y,
           seq, tgt, inv_freq, g_ap, g_ao, g_mp, g_mo, g_fi, y_v, hid_v, wq_v, wk_v, wv_v, kb, vb, wo_v, wg_v, wu_v, wd_v, emb_v,
           act, s1, s2, r1, r2, m1, xs, gs, gt, h_v, fz, fx,
           lsem, ssem, r_rs, z_rs, a_rs, b_rs, d_rs, f_rs):
    N, D = hid.shape
    HD = wk.shape[1]
    FH = wg_v.shape[1]
    CTX = kc.shape[1]
    VL = emb.shape[0]
    L = D // 128
    R = 2 * NT
    LP = s1.shape[0] // R
    PZ = NZ // 2
    t = lax.axis_index('t')
    v = lax.axis_index('v')
    c = lax.rem(v, 2)
    y = lax.rem(v // 2, NY)
    z = v // (2 * NY)
    me_r = 2 * t + c

    def dev(tt, zz, yy, cc):
        return {'t': tt, 'v': (zz * NY + yy) * 2 + cc}

    partner = dev(t, z, y, 1 - c)
    near_first = sorted(range(1, NZ), key=lambda k: min(k, NZ - k))
    ring = [k for k in (1, NT - 1, 2) if 0 < k < NT]
    ring = sorted(set(ring), key=ring.index)
    z_order = [k for k in near_first if k in (1, NZ - 1)] + [k for k in near_first[::-1] if k not in (1, NZ - 1)]
    z_peers = [(lax.rem(z + k, NZ), dev(t, lax.rem(z + k, NZ), y, c)) for k in z_order]
    r_peers = []
    for k in sorted(range(1, R), key=lambda k: -min(k // 2, NT - k // 2)):
        rr = lax.rem(me_r + k, R)
        r_peers.append((rr, dev(rr // 2, z, y, lax.rem(rr, 2))))
    own_a = jnp.where(c == 0, y, t)
    own_b = jnp.where(c == 0, t, y)
    a_peers = []
    b_peers = []
    for k in ring:
        a_peers.append((lax.rem(own_a + k, NT), dev(lax.rem(t + k * c, NT), z, lax.rem(y + k * (1 - c), NY), c)))
        b_peers.append((lax.rem(own_b + k, NT), dev(lax.rem(t + k * (1 - c), NT), z, lax.rem(y + k * c, NY), c)))
    zc_peers = []
    for dz in near_first[::-1] + [0]:
        for dc in (0, 1):
            if dz or dc:
                zz, cc = lax.rem(z + dz, NZ), (c if dc == 0 else 1 - c)
                zc_peers.append((zz * 2 + cc, dev(t, zz, y, cc)))
    xy_peers = []
    steps = [(dx, dy) for dx in range(NT) for dy in range(NY) if dx or dy]
    for dx, dy in sorted(steps, key=lambda s: -min(s[0], NT - s[0]) - min(s[1], NY - s[1])):
        xx, yy = lax.rem(t + dx, NT), lax.rem(y + dy, NY)
        xy_peers.append((xx * NY + yy, dev(xx, z, yy, c)))

    def token_of(r):
        rx, rc = r // 2, r % 2
        if rc == 0:
            return (rx * NT + y) * NZ + z
        return ((NT + y) * NT + rx) * NZ + z

    tokens = [token_of(r) for r in range(R)]
    chd = pl.ds(pl.multiple_of(c * HD, HD), HD)
    cfh = pl.ds(pl.multiple_of(c * FH, 128), FH)
    loads = {}

    def load(name, src, dst, sem):
        loads[name] = pltpu.make_async_copy(src, dst, sem)
        loads[name].start()

    load('seq', seq_h, seq, lsem.at[11])
    load('freq', freq_h, inv_freq, lsem.at[12])
    load('ap', ap_h, g_ap, lsem.at[13])
    load('hid', hid, hid_v, lsem.at[0])
    load('wq', wq.at[:, chd], wq_v, lsem.at[1])
    load('wk', wk, wk_v, lsem.at[2])
    load('wv', wv, wv_v, lsem.at[3])
    for r in range(R):
        load('k%d' % r, kc.at[tokens[r]], kb.at[r], lsem.at[9])
    for r in range(R):
        load('v%d' % r, vc.at[tokens[r]], vb.at[r], lsem.at[10])
    for i, (src, dst) in enumerate(((tgt_h, tgt), (ao_h, g_ao), (mp_h, g_mp), (mo_h, g_mo), (fi_h, g_fi))):
        load('small%d' % i, src, dst, lsem.at[14 + i])
    load('wo', wo.at[chd], wo_v, lsem.at[4])

    barrier = pltpu.get_barrier_semaphore()
    greeted = [d for _, d in zc_peers + xy_peers]
    for k in range(1, NT):
        greeted.append(dev(lax.rem(t + k, NT), z, y, 1 - c))
    for d in greeted:
        pl.semaphore_signal(barrier, inc=1, device_id=d, device_id_type=MESH)

    def send(src, dst, lane, recv_sem, device):
        pltpu.make_async_remote_copy(
            src_ref=src, dst_ref=dst, send_sem=ssem.at[lane], recv_sem=recv_sem,
            device_id=device, device_id_type=MESH).start()

    def all_sent(ref, lane):
        pltpu.make_async_remote_copy(
            src_ref=ref, dst_ref=ref, send_sem=ssem.at[lane], recv_sem=z_rs.at[0],
            device_id=partner, device_id_type=MESH).wait_send()

    def arrived(ref, recv_sem):
        pltpu.make_async_remote_copy(
            src_ref=ref, dst_ref=ref, send_sem=ssem.at[0], recv_sem=recv_sem,
            device_id=partner, device_id_type=MESH).wait_recv()

    for buf in (s1, s2, xs, gs):
        buf[...] = jnp.zeros_like(buf)
    def slot(k):
        return pl.ds(pl.multiple_of(k * LP, 8), LP)

    def to_rows(buf, values, at):
        for i in range(values.shape[1] // 128):
            buf[pl.ds(at + i, R, stride=LP), :] = values[:, 128 * i:128 * (i + 1)]

    others = pl.ds(0, (R - 1) * LP)

    def reduce_rows(src, dst, lane):
        for k, d in r_peers:
            send(src.at[slot(k)], dst.at[slot(me_r)], lane, r_rs.at[lane], d)
        dst[slot(me_r), :] = src[slot(me_r), :]
        arrived(dst.at[others], r_rs.at[lane])
        row = dst[pl.ds(0, LP), :]
        for k in range(1, R):
            row = row + dst[pl.ds(k * LP, LP), :]
        return row

    def rms_row(row, i):
        mean_sq = jnp.sum(jnp.sum(row * row, axis=0, keepdims=True), axis=1, keepdims=True) * (1.0 / D)
        return row * lax.rsqrt(mean_sq + NORM_EPS) * (1.0 + gs[pl.ds(i * LP, LP), :])

    rr = lax.broadcasted_iota(jnp.int32, (R, 1), 0)
    rx, rc = lax.shift_right_logical(rr, 1), jnp.bitwise_and(rr, 1)
    token_col = jnp.where(rc == 0, (rx * NT + y) * NZ + z, ((NT + y) * NT + rx) * NZ + z)
    pick = jnp.where(lax.broadcasted_iota(jnp.int32, (R, N), 1) == token_col, 1.0, 0.0).astype(BF16)
    loads['seq'].wait()
    loads['freq'].wait()
    loads['ap'].wait()
    pos = jnp.zeros((R, 1), jnp.int32)
    for r in range(R):
        pos = jnp.where(rr == r, seq[tokens[r]], pos)
    angles = pos.astype(F32) * inv_freq[...]
    cos_t = jnp.cos(angles)
    sin_t = jnp.sin(angles)

    def rotary(values):
        low, high = values[:, :HD // 2], values[:, HD // 2:]
        return jnp.concatenate([low * cos_t - high * sin_t, high * cos_t + low * sin_t], axis=-1).astype(BF16)

    loads['hid'].wait()
    x = dot(pick, hid_v[...])
    normed = rms(x, g_ap[...].astype(F32).reshape(1, D)).astype(BF16)
    to_rows(xs, x, 0)
    for name in ('wq', 'wk', 'wv'):
        loads[name].wait()
    q_rot = rotary(dot(normed, wq_v[...]))
    k_rot = rotary(dot(normed, wk_v[...]))
    v_new = dot(normed, wv_v[...]).astype(BF16)
    scale = HD ** -0.5
    pltpu.make_async_copy(kb, kb, lsem.at[9]).wait()
    load('wg', wg.at[:, cfh], wg_v, lsem.at[5])
    load('wu', wu.at[:, cfh], wu_v, lsem.at[6])
    load('wd', wd.at[cfh], wd_v, lsem.at[7])
    load('emb', emb, emb_v, lsem.at[8])
    scores = [dot_nt(q_rot, kb[r]) for r in range(R)]
    s_cache = scores[0]
    for r in range(1, R):
        s_cache = jnp.where(rr == r, scores[r], s_cache)
    s_new = jnp.sum(q_rot.astype(F32) * k_rot.astype(F32), axis=-1, keepdims=True) * scale
    s_cache = ATTN_CAP * jnp.tanh(s_cache * scale / ATTN_CAP)
    s_new = ATTN_CAP * jnp.tanh(s_new / ATTN_CAP)
    valid = lax.broadcasted_iota(jnp.int32, (R, CTX), 1) < pos
    s_cache = jnp.where(valid, s_cache, -1e30)
    row_max = jnp.maximum(jnp.max(s_cache, axis=-1, keepdims=True), s_new)
    p_cache = jnp.exp(s_cache - row_max)
    p_new = jnp.exp(s_new - row_max)
    denominator = jnp.sum(p_cache, axis=-1, keepdims=True) + p_new
    p_bf = p_cache.astype(BF16)
    pltpu.make_async_copy(vb, vb, lsem.at[10]).wait()
    parts = [dot(p_bf, vb[r]) for r in range(R)]
    weighted = parts[0]
    for r in range(1, R):
        weighted = jnp.where(rr == r, parts[r], weighted)
    weighted = weighted + p_new.astype(BF16).astype(F32) * v_new.astype(F32)
    attn_vec = (weighted / denominator).astype(BF16)
    loads['wo'].wait()
    to_rows(s1, dot(attn_vec, wo_v[...]), 0)
    for i in range(5):
        loads['small%d' % i].wait()
    for i, gain in enumerate((g_ao, g_mo)):
        gain_row = gain[...].astype(F32).reshape(1, D)
        for l in range(L):
            gs[pl.ds(i * LP + l, 1), :] = gain_row[:, 128 * l:128 * (l + 1)]

    pl.semaphore_wait(barrier, len(greeted))
    row = reduce_rows(s1, r1, 0)
    mid_row = (xs[slot(me_r), :] + rms_row(row, 0)).astype(BF16).astype(F32)
    m1[slot(me_r), :] = mid_row
    for _, d in r_peers:
        send(m1.at[slot(me_r)], m1.at[slot(me_r)], 1, r_rs.at[1], d)
    arrived(m1.at[others], r_rs.at[1])
    mid = jnp.concatenate([m1[pl.ds(l, R, stride=LP), :] for l in range(L)], axis=-1)
    mlp_in = rms(mid, g_mp[...].astype(F32).reshape(1, D)).astype(BF16)

    loads['wg'].wait()
    loads['wu'].wait()
    width = 384 if FH % 384 == 0 else 128
    for j in range(FH // width):
        cols = pl.ds(j * width, width)
        gate = dot(mlp_in, wg_v[:, cols])
        up = dot(mlp_in, wu_v[:, cols])
        act[:, cols] = (jax.nn.gelu(gate, approximate=True) * up).astype(BF16)
    loads['wd'].wait()
    width = 768 if D % 768 == 0 else 128
    for j in range(D // width):
        to_rows(s2, dot(act[...], wd_v[:, pl.ds(j * width, width)]), j * (width // 128))
    row = reduce_rows(s2, r2, 2)
    y_row = (m1[slot(me_r), :] + rms_row(row, 1)).astype(BF16).astype(F32)

    def pair(core, b, a, q):
        return pl.ds((((core * NT + b) * NT + a) * NZ + 2 * q) * L, 2 * L)

    def single(zz):
        return pl.ds((((c * NT + own_b) * NT + own_a) * NZ + zz) * L, L)

    me_at = (((c * NT + own_b) * NT + own_a) * NZ + z) * L
    for l in range(L):
        gt[me_at + l] = y_row[l:l + 1, :]
    my_q = z // 2
    for _, d in z_peers:
        send(gt.at[single(z)], gt.at[single(z)], 3, z_rs.at[my_q], d)

    def rows_of(count):
        return gt.at[pl.ds(0, count * L)]

    def to_b_and_core(a, q, late):
        here = gt.at[pair(c, own_b, a, q)]
        for _, d in b_peers:
            send(here, here, 5, b_rs.at[(own_b * PZ + q) * 2 + late], d)
        send(here, here, 6, d_rs.at[own_b], partner)

    def own_pair(dq):
        q = lax.rem(my_q + dq, PZ)
        arrived(rows_of(1 if dq == 0 else 2), z_rs.at[q])
        here = gt.at[pair(c, own_b, own_a, q)]
        for _, d in a_peers:
            send(here, here, 4, a_rs.at[q], d)
        to_b_and_core(own_a, q, 0)

    def first_axis(dq):
        q = lax.rem(my_q + dq, PZ)
        arrived(rows_of(2 * (NT - 1)), a_rs.at[q])
        for a, _ in a_peers:
            to_b_and_core(a, q, 1)

    if PZ == 4:
        own_pair(0)
        own_pair(1)
        own_pair(3)
        first_axis(0)
        own_pair(2)
        first_axis(1)
        first_axis(3)
        first_axis(2)
    else:
        for dq in range(PZ):
            own_pair(dq)
        for dq in range(PZ):
            first_axis(dq)
    order = [0, 1, 3, 2] if PZ == 4 else list(range(PZ))

    g_fi_row = 1.0 + g_fi[...].astype(F32).reshape(1, D)
    unit = 16 if NT * NZ % 16 == 0 else NT * NZ

    def final_norm(core, b):
        def body(i, carry):
            first = (core * NT + b) * (NT * NZ) + i * unit
            tiles = []
            for l in range(L):
                tiles.append(jnp.concatenate(
                    [gt[pl.ds((first + j) * L + l, NZ, stride=L), 0, :] for j in range(0, unit, NZ)], axis=0))
            square = tiles[0] * tiles[0]
            for l in range(1, L):
                square = square + tiles[l] * tiles[l]
            inv = lax.rsqrt(jnp.sum(square, axis=-1, keepdims=True) * (1.0 / D) + NORM_EPS)
            rows = pl.ds(pl.multiple_of(first, unit), unit)
            for l in range(L):
                cols = slice(128 * l, 128 * (l + 1))
                y_v[rows, cols] = tiles[l].astype(BF16)
                h_v[rows, cols] = (tiles[l] * inv * g_fi_row[:, cols]).astype(BF16)
            return carry
        lax.fori_loop(0, NT * NZ // unit, body, 0, unroll=True)

    def second_axis(b, dq, late):
        q = lax.rem(my_q + dq, PZ)
        lanes = [a for a, _ in a_peers] if late else [own_a]
        arrived(rows_of(2 * len(lanes)), b_rs.at[(b * PZ + q) * 2 + late])
        for a in lanes:
            piece = gt.at[pair(c, b, a, q)]
            send(piece, piece, 6, d_rs.at[b], partner)

    def other_core(k):
        b = lax.rem(own_a + k, NT)
        arrived(rows_of(NT * NZ), d_rs.at[b])
        final_norm(1 - c, b)

    final_norm(c, own_b)
    for dq in order:
        for b, _ in b_peers:
            second_axis(b, dq, 0)
    other_core(0)
    for dq in order:
        for b, _ in b_peers:
            second_axis(b, dq, 1)
    for b, _ in b_peers:
        final_norm(c, b)
    for k in ring:
        other_core(k)

    load('y', y_v, out_y, lsem.at[19])

    loads['emb'].wait()
    rows_at = 0
    total = jnp.zeros((1, N), F32)
    hit = jnp.zeros((1, N), F32)
    target = tgt[...].reshape(1, N) - (v * NT + t) * VL
    while rows_at < VL:
        size = min(256, VL - rows_at)
        logits = dot_nt(emb_v[pl.ds(rows_at, size), :], h_v[...])
        capped = FINAL_CAP * jnp.tanh(logits * (1.0 / FINAL_CAP))
        total = total + jnp.sum(jnp.exp(capped), axis=0, keepdims=True)
        ids = rows_at + lax.broadcasted_iota(jnp.int32, (size, N), 0)
        hit = hit + jnp.sum(jnp.where(ids == target, capped, 0.0), axis=0, keepdims=True)
        rows_at += size
    stats = jnp.concatenate([total, hit], axis=0)

    for i, (buf, me, peers) in enumerate(((fz, z * 2 + c, zc_peers), (fx, t * NY + y, xy_peers))):
        buf[me] = stats
        for _, d in peers:
            send(buf.at[me], buf.at[me], 7 + i, f_rs.at[i], d)
        arrived(buf.at[pl.ds(0, len(peers))], f_rs.at[i])
        stats = buf[0]
        for k in range(1, buf.shape[0]):
            stats = stats + buf[k]
    out_lp[...] = stats[1:2, :] - jnp.log(stats[0:1, :])
    loads['y'].wait()
    for lane, ref in enumerate((
            s1.at[others], m1.at[others], s2.at[others], rows_of(NZ - 1), rows_of(PZ * 2 * (NT - 1)),
            rows_of(NT * PZ * 2 * (NT - 1)), rows_of(NT * NT * NZ), fz.at[pl.ds(0, len(zc_peers))],
            fx.at[pl.ds(0, len(xy_peers))])):
        all_sent(ref, lane)


def hand_on(parts, lp_in, y_in, lp_out, y_out, lp_v, y_v, sems):
    rows = y_v.shape[1]
    first = pltpu.make_async_copy(lp_in, lp_v, sems.at[0])
    first.start()
    into = [pltpu.make_async_copy(y_in.at[pl.ds(i * rows, rows)], y_v.at[i], sems.at[1 + i]) for i in range(parts)]
    for copy in into:
        copy.start()
    first.wait()
    out = [pltpu.make_async_copy(lp_v, lp_out, sems.at[1 + parts])]
    out[0].start()
    for i in range(parts):
        into[i].wait()
        out.append(pltpu.make_async_copy(y_v.at[i], y_out.at[pl.ds(i * rows, rows)], sems.at[2 + parts + i]))
        out[-1].start()
    for copy in out:
        copy.wait()


def solution(mesh):
    NT = mesh.shape['t']
    V = mesh.shape['v']
    NY = NT
    NZ = V // (2 * NY)
    in_specs = (P(), P(), P(), P(), P(None, 't'), P(None, 't'), P(None, 't'), P('t', None), P(), P(), P(None, 't'), P(None, 't'), P('t', None), P(), P(), P(None, None, 't', None), P(None, None, 't', None), P(('v', 't'), None))

    def local_step(hidden_in, seq_lens, target, g_attn_pre, w_q, w_k, w_v, w_o, g_attn_post, g_mlp_pre, w_gate, w_up, w_down, g_mlp_post, g_final, k_cache, v_cache, embed_table):
        N, D = hidden_in.shape
        CTX, _, HD = k_cache.shape[1:]
        FH = w_gate.shape[1] // 2
        VL = embed_table.shape[0]
        R = 2 * NT
        LP = (D // 128 + 7) // 8 * 8
        inv_freq = (ROPE_BASE ** (-2.0 * np.arange(HD // 2, dtype=np.float32) / HD)).astype(np.float32).reshape(1, HD // 2)
        vmem = pl.BlockSpec(memory_space=pltpu.VMEM)
        PZ = NZ // 2
        dma = pltpu.SemaphoreType.DMA
        rows = pltpu.VMEM((R * LP, 128), F32)
        lp, hidden_out = pl.pallas_call(
            functools.partial(kernel, NT, NY, NZ),
            name='decode_step',
            out_shape=(jax.ShapeDtypeStruct((1, N), F32), jax.ShapeDtypeStruct((N, D), BF16)),
            in_specs=[pl.BlockSpec(memory_space=pltpu.HBM)] * 19,
            out_specs=(vmem, pl.BlockSpec(memory_space=pltpu.HBM)),
            scratch_shapes=[
                pltpu.SMEM((N,), jnp.int32), pltpu.VMEM((N,), jnp.int32), pltpu.VMEM((1, HD // 2), F32)]
            + [pltpu.VMEM((D,), BF16)] * 5 + [
                pltpu.VMEM((N, D), BF16), pltpu.VMEM((N, D), BF16), pltpu.VMEM((D, HD), BF16), pltpu.VMEM((D, HD), BF16), pltpu.VMEM((D, HD), BF16),
                pltpu.VMEM((R, CTX, HD), BF16), pltpu.VMEM((R, CTX, HD), BF16), pltpu.VMEM((HD, D), BF16),
                pltpu.VMEM((D, FH), BF16), pltpu.VMEM((D, FH), BF16), pltpu.VMEM((FH, D), BF16), pltpu.VMEM((VL, D), BF16),
                pltpu.VMEM((R, FH), BF16), rows, rows, rows, rows, rows, rows, pltpu.VMEM((2 * LP, 128), F32),
                pltpu.VMEM((N * (D // 128), 1, 128), F32), pltpu.VMEM((N, D), BF16),
                pltpu.VMEM((2 * NZ, 2, N), F32), pltpu.VMEM((NT * NY, 2, N), F32),
                dma((20,)), dma((9,)), dma((3,)), dma((PZ,)), dma((PZ,)), dma((NT * PZ * 2,)), dma((NT,)), dma((2,)),
            ],
            compiler_params=pltpu.CompilerParams(
                collective_id=0, has_side_effects=True, vmem_limit_bytes=VMEM_LIMIT),
        )(seq_lens, hidden_in, target, inv_freq, g_attn_pre, g_attn_post, g_mlp_pre, g_mlp_post, g_final,
          w_q, w_k, w_v, w_o, w_gate, w_up, w_down,
          k_cache.reshape(N, CTX, HD), v_cache.reshape(N, CTX, HD), embed_table)
        parts = 4 if N % 64 == 0 else 1
        hbm = pl.BlockSpec(memory_space=pltpu.HBM)
        lp, hidden_out = pl.pallas_call(
            functools.partial(hand_on, parts),
            name='hand_on',
            out_shape=(jax.ShapeDtypeStruct((1, N), F32), jax.ShapeDtypeStruct((N, D), BF16)),
            in_specs=[hbm, hbm],
            out_specs=(hbm, hbm),
            scratch_shapes=[pltpu.VMEM((1, N), F32), pltpu.VMEM((parts, N // parts, D), BF16), dma((2 + 2 * parts,))],
            compiler_params=pltpu.CompilerParams(vmem_limit_bytes=VMEM_LIMIT),
        )(lp, hidden_out)
        return lp.reshape(N), hidden_out

    return jax.shard_map(local_step, mesh=mesh, in_specs=in_specs, out_specs=(P(), P()), check_vma=False)
```

```python
import functools

import jax
import jax.numpy as jnp
import numpy as np
from jax import lax
from jax.experimental import pallas as pl
from jax.experimental.pallas import tpu as pltpu
from jax.sharding import PartitionSpec as P

ATTN_CAP = 50.0
FINAL_CAP = 30.0
NORM_EPS = 1e-6
ROPE_BASE = 10000.0
MESH = pl.DeviceIdType.MESH
F32 = jnp.float32
BF16 = jnp.bfloat16
VMEM_LIMIT = 60 * 1024 * 1024


def dot(a, b):
    return jnp.dot(a, b, preferred_element_type=F32)


def dot_nt(a, b):
    return lax.dot_general(a, b, (((1,), (1,)), ((), ())), preferred_element_type=F32)


def rms(values, gain):
    mean_sq = jnp.mean(values * values, axis=-1, keepdims=True)
    return values * lax.rsqrt(mean_sq + NORM_EPS) * (1.0 + gain)


def kernel(NT, NY, NZ, seq_h, hid, tgt_h, freq_h, ap_h, ao_h, mp_h, mo_h, fi_h, wq, wk, wv, wo, wg, wu, wd, kc, vc, emb,
           out_lp, out_y,
           seq, tgt, inv_freq, g_ap, g_ao, g_mp, g_mo, g_fi, y_v, hid_v, wq_v, wk_v, wv_v, kb, vb, wo_v, wg_v, wu_v, wd_v, emb_v,
           act, s1, s2, r1, r2, m1, xs, gs, gt, h_v, fz, fx,
           lsem, ssem, r_rs, z_rs, a_rs, b_rs, d_rs, f_rs):
    N, D = hid.shape
    HD = wk.shape[1]
    FH = wg_v.shape[1]
    CTX = kc.shape[1]
    VL = emb.shape[0]
    L = D // 128
    R = 2 * NT
    LP = s1.shape[0] // R
    PZ = NZ // 2
    t = lax.axis_index('t')
    v = lax.axis_index('v')
    c = lax.rem(v, 2)
    y = lax.rem(v // 2, NY)
    z = v // (2 * NY)
    me_r = 2 * t + c

    def dev(tt, zz, yy, cc):
        return {'t': tt, 'v': (zz * NY + yy) * 2 + cc}

    partner = dev(t, z, y, 1 - c)
    near_first = sorted(range(1, NZ), key=lambda k: min(k, NZ - k))
    ring = [k for k in (1, NT - 1, 2) if 0 < k < NT]
    ring = sorted(set(ring), key=ring.index)
    z_order = [k for k in near_first if k in (1, NZ - 1)] + [k for k in near_first[::-1] if k not in (1, NZ - 1)]
    z_peers = [(lax.rem(z + k, NZ), dev(t, lax.rem(z + k, NZ), y, c)) for k in z_order]
    r_peers = []
    for k in sorted(range(1, R), key=lambda k: -min(k // 2, NT - k // 2)):
        rr = lax.rem(me_r + k, R)
        r_peers.append((rr, dev(rr // 2, z, y, lax.rem(rr, 2))))
    own_a = jnp.where(c == 0, y, t)
    own_b = jnp.where(c == 0, t, y)
    a_peers = []
    b_peers = []
    for k in ring:
        a_peers.append((lax.rem(own_a + k, NT), dev(lax.rem(t + k * c, NT), z, lax.rem(y + k * (1 - c), NY), c)))
        b_peers.append((lax.rem(own_b + k, NT), dev(lax.rem(t + k * (1 - c), NT), z, lax.rem(y + k * c, NY), c)))
    zc_peers = []
    for dz in near_first[::-1] + [0]:
        for dc in (0, 1):
            if dz or dc:
                zz, cc = lax.rem(z + dz, NZ), (c if dc == 0 else 1 - c)
                zc_peers.append((zz * 2 + cc, dev(t, zz, y, cc)))
    xy_peers = []
    steps = [(dx, dy) for dx in range(NT) for dy in range(NY) if dx or dy]
    for dx, dy in sorted(steps, key=lambda s: -min(s[0], NT - s[0]) - min(s[1], NY - s[1])):
        xx, yy = lax.rem(t + dx, NT), lax.rem(y + dy, NY)
        xy_peers.append((xx * NY + yy, dev(xx, z, yy, c)))

    def token_of(r):
        rx, rc = r // 2, r % 2
        if rc == 0:
            return (rx * NT + y) * NZ + z
        return ((NT + y) * NT + rx) * NZ + z

    tokens = [token_of(r) for r in range(R)]
    chd = pl.ds(pl.multiple_of(c * HD, HD), HD)
    cfh = pl.ds(pl.multiple_of(c * FH, 128), FH)
    loads = {}

    def load(name, src, dst, sem):
        loads[name] = pltpu.make_async_copy(src, dst, sem)
        loads[name].start()

    load('seq', seq_h, seq, lsem.at[11])
    load('freq', freq_h, inv_freq, lsem.at[12])
    load('ap', ap_h, g_ap, lsem.at[13])
    load('hid', hid, hid_v, lsem.at[0])
    load('wq', wq.at[:, chd], wq_v, lsem.at[1])
    load('wk', wk, wk_v, lsem.at[2])
    load('wv', wv, wv_v, lsem.at[3])
    for r in range(R):
        load('k%d' % r, kc.at[tokens[r]], kb.at[r], lsem.at[9])
    for r in range(R):
        load('v%d' % r, vc.at[tokens[r]], vb.at[r], lsem.at[10])
    for i, (src, dst) in enumerate(((tgt_h, tgt), (ao_h, g_ao), (mp_h, g_mp), (mo_h, g_mo), (fi_h, g_fi))):
        load('small%d' % i, src, dst, lsem.at[14 + i])
    load('wo', wo.at[chd], wo_v, lsem.at[4])

    barrier = pltpu.get_barrier_semaphore()
    greeted = [d for _, d in zc_peers + xy_peers]
    for k in range(1, NT):
        greeted.append(dev(lax.rem(t + k, NT), z, y, 1 - c))
    for d in greeted:
        pl.semaphore_signal(barrier, inc=1, device_id=d, device_id_type=MESH)

    def send(src, dst, lane, recv_sem, device):
        pltpu.make_async_remote_copy(
            src_ref=src, dst_ref=dst, send_sem=ssem.at[lane], recv_sem=recv_sem,
            device_id=device, device_id_type=MESH).start()

    def all_sent(ref, lane):
        pltpu.make_async_remote_copy(
            src_ref=ref, dst_ref=ref, send_sem=ssem.at[lane], recv_sem=z_rs.at[0],
            device_id=partner, device_id_type=MESH).wait_send()

    def arrived(ref, recv_sem):
        pltpu.make_async_remote_copy(
            src_ref=ref, dst_ref=ref, send_sem=ssem.at[0], recv_sem=recv_sem,
            device_id=partner, device_id_type=MESH).wait_recv()

    for buf in (s1, s2, xs, gs):
        buf[...] = jnp.zeros_like(buf)
    def slot(k):
        return pl.ds(pl.multiple_of(k * LP, 8), LP)

    per = L // (LP // 8)

    def at_row(l):
        return l // per * 8 + l % per

    def to_rows(buf, values, at):
        for i in range(values.shape[1] // 128):
            buf[pl.ds(at_row(at + i), R, stride=LP), :] = values[:, 128 * i:128 * (i + 1)]

    others = pl.ds(0, (R - 1) * LP)

    def send_group(src, dst, lane, group):
        def part(k):
            return pl.ds(pl.multiple_of(k * LP + 8 * group, 8), 8)
        for k, d in r_peers:
            send(src.at[part(k)], dst.at[part(me_r)], lane, r_rs.at[lane], d)

    def reduce_rows(src, dst, lane):
        dst[slot(me_r), :] = src[slot(me_r), :]
        arrived(dst.at[others], r_rs.at[lane])
        row = dst[pl.ds(0, LP), :]
        for k in range(1, R):
            row = row + dst[pl.ds(k * LP, LP), :]
        return row

    def rms_row(row, i):
        mean_sq = jnp.sum(jnp.sum(row * row, axis=0, keepdims=True), axis=1, keepdims=True) * (1.0 / D)
        return row * lax.rsqrt(mean_sq + NORM_EPS) * (1.0 + gs[pl.ds(i * LP, LP), :])

    rr = lax.broadcasted_iota(jnp.int32, (R, 1), 0)
    rx, rc = lax.shift_right_logical(rr, 1), jnp.bitwise_and(rr, 1)
    token_col = jnp.where(rc == 0, (rx * NT + y) * NZ + z, ((NT + y) * NT + rx) * NZ + z)
    pick = jnp.where(lax.broadcasted_iota(jnp.int32, (R, N), 1) == token_col, 1.0, 0.0).astype(BF16)
    loads['seq'].wait()
    loads['freq'].wait()
    loads['ap'].wait()
    pos = jnp.zeros((R, 1), jnp.int32)
    for r in range(R):
        pos = jnp.where(rr == r, seq[tokens[r]], pos)
    angles = pos.astype(F32) * inv_freq[...]
    cos_t = jnp.cos(angles)
    sin_t = jnp.sin(angles)

    def rotary(values):
        low, high = values[:, :HD // 2], values[:, HD // 2:]
        return jnp.concatenate([low * cos_t - high * sin_t, high * cos_t + low * sin_t], axis=-1).astype(BF16)

    loads['hid'].wait()
    x = dot(pick, hid_v[...])
    normed = rms(x, g_ap[...].astype(F32).reshape(1, D)).astype(BF16)
    to_rows(xs, x, 0)
    for name in ('wq', 'wk', 'wv'):
        loads[name].wait()
    q_rot = rotary(dot(normed, wq_v[...]))
    k_rot = rotary(dot(normed, wk_v[...]))
    v_new = dot(normed, wv_v[...]).astype(BF16)
    scale = HD ** -0.5
    pltpu.make_async_copy(kb, kb, lsem.at[9]).wait()
    load('wg', wg.at[:, cfh], wg_v, lsem.at[5])
    load('wu', wu.at[:, cfh], wu_v, lsem.at[6])
    load('wd', wd.at[cfh], wd_v, lsem.at[7])
    load('emb', emb, emb_v, lsem.at[8])
    scores = [dot_nt(q_rot, kb[r]) for r in range(R)]
    s_cache = scores[0]
    for r in range(1, R):
        s_cache = jnp.where(rr == r, scores[r], s_cache)
    s_new = jnp.sum(q_rot.astype(F32) * k_rot.astype(F32), axis=-1, keepdims=True) * scale
    s_cache = ATTN_CAP * jnp.tanh(s_cache * scale / ATTN_CAP)
    s_new = ATTN_CAP * jnp.tanh(s_new / ATTN_CAP)
    valid = lax.broadcasted_iota(jnp.int32, (R, CTX), 1) < pos
    s_cache = jnp.where(valid, s_cache, -1e30)
    row_max = jnp.maximum(jnp.max(s_cache, axis=-1, keepdims=True), s_new)
    p_cache = jnp.exp(s_cache - row_max)
    p_new = jnp.exp(s_new - row_max)
    denominator = jnp.sum(p_cache, axis=-1, keepdims=True) + p_new
    p_bf = p_cache.astype(BF16)
    pltpu.make_async_copy(vb, vb, lsem.at[10]).wait()
    parts = [dot(p_bf, vb[r]) for r in range(R)]
    weighted = parts[0]
    for r in range(1, R):
        weighted = jnp.where(rr == r, parts[r], weighted)
    weighted = weighted + p_new.astype(BF16).astype(F32) * v_new.astype(F32)
    attn_vec = (weighted / denominator).astype(BF16)
    loads['wo'].wait()
    to_rows(s1, dot(attn_vec, wo_v[...]), 0)
    for i in range(5):
        loads['small%d' % i].wait()
    for i, gain in enumerate((g_ao, g_mo)):
        gain_row = gain[...].astype(F32).reshape(1, D)
        for l in range(L):
            gs[pl.ds(i * LP + at_row(l), 1), :] = gain_row[:, 128 * l:128 * (l + 1)]

    pl.semaphore_wait(barrier, len(greeted))
    for k, d in r_peers:
        send(s1.at[slot(k)], r1.at[slot(me_r)], 0, r_rs.at[0], d)
    row = reduce_rows(s1, r1, 0)
    mid_row = (xs[slot(me_r), :] + rms_row(row, 0)).astype(BF16).astype(F32)
    m1[slot(me_r), :] = mid_row
    for _, d in r_peers:
        send(m1.at[slot(me_r)], m1.at[slot(me_r)], 1, r_rs.at[1], d)
    arrived(m1.at[others], r_rs.at[1])
    mid = jnp.concatenate([m1[pl.ds(at_row(l), R, stride=LP), :] for l in range(L)], axis=-1)
    mlp_in = rms(mid, g_mp[...].astype(F32).reshape(1, D)).astype(BF16)

    loads['wg'].wait()
    loads['wu'].wait()
    width = 384 if FH % 384 == 0 else 128
    for j in range(FH // width):
        cols = pl.ds(j * width, width)
        gate = dot(mlp_in, wg_v[:, cols])
        up = dot(mlp_in, wu_v[:, cols])
        act[:, cols] = (jax.nn.gelu(gate, approximate=True) * up).astype(BF16)
    loads['wd'].wait()
    for j in range(LP // 8):
        to_rows(s2, dot(act[...], wd_v[:, pl.ds(j * per * 128, per * 128)]), j * per)
        send_group(s2, r2, 2, j)
    row = reduce_rows(s2, r2, 2)
    y_row = (m1[slot(me_r), :] + rms_row(row, 1)).astype(BF16).astype(F32)

    def pair(core, b, a, q):
        return pl.ds((((core * NT + b) * NT + a) * NZ + 2 * q) * L, 2 * L)

    def single(zz):
        return pl.ds((((c * NT + own_b) * NT + own_a) * NZ + zz) * L, L)

    me_at = (((c * NT + own_b) * NT + own_a) * NZ + z) * L
    for l in range(L):
        gt[me_at + l] = y_row[at_row(l):at_row(l) + 1, :]
    my_q = z // 2
    for _, d in z_peers:
        send(gt.at[single(z)], gt.at[single(z)], 3, z_rs.at[my_q], d)

    def rows_of(count):
        return gt.at[pl.ds(0, count * L)]

    def to_b_and_core(a, q, late):
        here = gt.at[pair(c, own_b, a, q)]
        for _, d in b_peers:
            send(here, here, 5, b_rs.at[(own_b * PZ + q) * 2 + late], d)
        send(here, here, 6, d_rs.at[own_b], partner)

    def own_pair(dq):
        q = lax.rem(my_q + dq, PZ)
        arrived(rows_of(1 if dq == 0 else 2), z_rs.at[q])
        here = gt.at[pair(c, own_b, own_a, q)]
        for _, d in a_peers:
            send(here, here, 4, a_rs.at[q], d)
        to_b_and_core(own_a, q, 0)

    def first_axis(dq):
        q = lax.rem(my_q + dq, PZ)
        arrived(rows_of(2 * (NT - 1)), a_rs.at[q])
        for a, _ in a_peers:
            to_b_and_core(a, q, 1)

    if PZ == 4:
        own_pair(0)
        own_pair(1)
        own_pair(3)
        first_axis(0)
        own_pair(2)
        first_axis(1)
        first_axis(3)
        first_axis(2)
    else:
        for dq in range(PZ):
            own_pair(dq)
        for dq in range(PZ):
            first_axis(dq)
    order = [0, 1, 3, 2] if PZ == 4 else list(range(PZ))

    g_fi_row = 1.0 + g_fi[...].astype(F32).reshape(1, D)
    unit = 16 if NT * NZ % 16 == 0 else NT * NZ

    def final_norm(core, b):
        def body(i, carry):
            first = (core * NT + b) * (NT * NZ) + i * unit
            tiles = []
            for l in range(L):
                tiles.append(jnp.concatenate(
                    [gt[pl.ds((first + j) * L + l, NZ, stride=L), 0, :] for j in range(0, unit, NZ)], axis=0))
            square = tiles[0] * tiles[0]
            for l in range(1, L):
                square = square + tiles[l] * tiles[l]
            inv = lax.rsqrt(jnp.sum(square, axis=-1, keepdims=True) * (1.0 / D) + NORM_EPS)
            rows = pl.ds(pl.multiple_of(first, unit), unit)
            for l in range(L):
                cols = slice(128 * l, 128 * (l + 1))
                y_v[rows, cols] = tiles[l].astype(BF16)
                h_v[rows, cols] = (tiles[l] * inv * g_fi_row[:, cols]).astype(BF16)
            return carry
        lax.fori_loop(0, NT * NZ // unit, body, 0, unroll=True)

    def second_axis(b, dq, late):
        q = lax.rem(my_q + dq, PZ)
        lanes = [a for a, _ in a_peers] if late else [own_a]
        arrived(rows_of(2 * len(lanes)), b_rs.at[(b * PZ + q) * 2 + late])
        for a in lanes:
            piece = gt.at[pair(c, b, a, q)]
            send(piece, piece, 6, d_rs.at[b], partner)

    def other_core(k):
        b = lax.rem(own_a + k, NT)
        arrived(rows_of(NT * NZ), d_rs.at[b])
        final_norm(1 - c, b)

    final_norm(c, own_b)
    for dq in order:
        for b, _ in b_peers:
            second_axis(b, dq, 0)
    other_core(0)
    for dq in order:
        for b, _ in b_peers:
            second_axis(b, dq, 1)
    for b, _ in b_peers:
        final_norm(c, b)
    for k in ring:
        other_core(k)

    load('y', y_v, out_y, lsem.at[19])

    loads['emb'].wait()
    rows_at = 0
    total = jnp.zeros((1, N), F32)
    hit = jnp.zeros((1, N), F32)
    target = tgt[...].reshape(1, N) - (v * NT + t) * VL
    while rows_at < VL:
        size = min(256, VL - rows_at)
        logits = dot_nt(emb_v[pl.ds(rows_at, size), :], h_v[...])
        capped = FINAL_CAP * jnp.tanh(logits * (1.0 / FINAL_CAP))
        total = total + jnp.sum(jnp.exp(capped), axis=0, keepdims=True)
        ids = rows_at + lax.broadcasted_iota(jnp.int32, (size, N), 0)
        hit = hit + jnp.sum(jnp.where(ids == target, capped, 0.0), axis=0, keepdims=True)
        rows_at += size
    stats = jnp.concatenate([total, hit], axis=0)

    for i, (buf, me, peers) in enumerate(((fz, z * 2 + c, zc_peers), (fx, t * NY + y, xy_peers))):
        buf[me] = stats
        for _, d in peers:
            send(buf.at[me], buf.at[me], 7 + i, f_rs.at[i], d)
        arrived(buf.at[pl.ds(0, len(peers))], f_rs.at[i])
        stats = buf[0]
        for k in range(1, buf.shape[0]):
            stats = stats + buf[k]
    out_lp[...] = stats[1:2, :] - jnp.log(stats[0:1, :])
    loads['y'].wait()
    for lane, ref in enumerate((
            s1.at[others], m1.at[others], s2.at[others], rows_of(NZ - 1), rows_of(PZ * 2 * (NT - 1)),
            rows_of(NT * PZ * 2 * (NT - 1)), rows_of(NT * NT * NZ), fz.at[pl.ds(0, len(zc_peers))],
            fx.at[pl.ds(0, len(xy_peers))])):
        all_sent(ref, lane)


def hand_on(parts, lp_in, y_in, lp_out, y_out, lp_v, y_v, sems):
    rows = y_v.shape[1]
    first = pltpu.make_async_copy(lp_in, lp_v, sems.at[0])
    first.start()
    into = [pltpu.make_async_copy(y_in.at[pl.ds(i * rows, rows)], y_v.at[i], sems.at[1 + i]) for i in range(parts)]
    for copy in into:
        copy.start()
    first.wait()
    out = [pltpu.make_async_copy(lp_v, lp_out, sems.at[1 + parts])]
    out[0].start()
    for i in range(parts):
        into[i].wait()
        out.append(pltpu.make_async_copy(y_v.at[i], y_out.at[pl.ds(i * rows, rows)], sems.at[2 + parts + i]))
        out[-1].start()
    for copy in out:
        copy.wait()


def solution(mesh):
    NT = mesh.shape['t']
    V = mesh.shape['v']
    NY = NT
    NZ = V // (2 * NY)
    in_specs = (P(), P(), P(), P(), P(None, 't'), P(None, 't'), P(None, 't'), P('t', None), P(), P(), P(None, 't'), P(None, 't'), P('t', None), P(), P(), P(None, None, 't', None), P(None, None, 't', None), P(('v', 't'), None))

    def local_step(hidden_in, seq_lens, target, g_attn_pre, w_q, w_k, w_v, w_o, g_attn_post, g_mlp_pre, w_gate, w_up, w_down, g_mlp_post, g_final, k_cache, v_cache, embed_table):
        N, D = hidden_in.shape
        CTX, _, HD = k_cache.shape[1:]
        FH = w_gate.shape[1] // 2
        VL = embed_table.shape[0]
        R = 2 * NT
        LP = 24 if D % 384 == 0 else (D // 128 + 7) // 8 * 8
        inv_freq = (ROPE_BASE ** (-2.0 * np.arange(HD // 2, dtype=np.float32) / HD)).astype(np.float32).reshape(1, HD // 2)
        vmem = pl.BlockSpec(memory_space=pltpu.VMEM)
        PZ = NZ // 2
        dma = pltpu.SemaphoreType.DMA
        rows = pltpu.VMEM((R * LP, 128), F32)
        lp, hidden_out = pl.pallas_call(
            functools.partial(kernel, NT, NY, NZ),
            name='decode_step',
            out_shape=(jax.ShapeDtypeStruct((1, N), F32), jax.ShapeDtypeStruct((N, D), BF16)),
            in_specs=[pl.BlockSpec(memory_space=pltpu.HBM)] * 19,
            out_specs=(vmem, pl.BlockSpec(memory_space=pltpu.HBM)),
            scratch_shapes=[
                pltpu.SMEM((N,), jnp.int32), pltpu.VMEM((N,), jnp.int32), pltpu.VMEM((1, HD // 2), F32)]
            + [pltpu.VMEM((D,), BF16)] * 5 + [
                pltpu.VMEM((N, D), BF16), pltpu.VMEM((N, D), BF16), pltpu.VMEM((D, HD), BF16), pltpu.VMEM((D, HD), BF16), pltpu.VMEM((D, HD), BF16),
                pltpu.VMEM((R, CTX, HD), BF16), pltpu.VMEM((R, CTX, HD), BF16), pltpu.VMEM((HD, D), BF16),
                pltpu.VMEM((D, FH), BF16), pltpu.VMEM((D, FH), BF16), pltpu.VMEM((FH, D), BF16), pltpu.VMEM((VL, D), BF16),
                pltpu.VMEM((R, FH), BF16), rows, rows, rows, rows, rows, rows, pltpu.VMEM((2 * LP, 128), F32),
                pltpu.VMEM((N * (D // 128), 1, 128), F32), pltpu.VMEM((N, D), BF16),
                pltpu.VMEM((2 * NZ, 2, N), F32), pltpu.VMEM((NT * NY, 2, N), F32),
                dma((20,)), dma((9,)), dma((3,)), dma((PZ,)), dma((PZ,)), dma((NT * PZ * 2,)), dma((NT,)), dma((2,)),
            ],
            compiler_params=pltpu.CompilerParams(
                collective_id=0, has_side_effects=True, vmem_limit_bytes=VMEM_LIMIT),
        )(seq_lens, hidden_in, target, inv_freq, g_attn_pre, g_attn_post, g_mlp_pre, g_mlp_post, g_final,
          w_q, w_k, w_v, w_o, w_gate, w_up, w_down,
          k_cache.reshape(N, CTX, HD), v_cache.reshape(N, CTX, HD), embed_table)
        parts = 4 if N % 64 == 0 else 1
        hbm = pl.BlockSpec(memory_space=pltpu.HBM)
        lp, hidden_out = pl.pallas_call(
            functools.partial(hand_on, parts),
            name='hand_on',
            out_shape=(jax.ShapeDtypeStruct((1, N), F32), jax.ShapeDtypeStruct((N, D), BF16)),
            in_specs=[hbm, hbm],
            out_specs=(hbm, hbm),
            scratch_shapes=[pltpu.VMEM((1, N), F32), pltpu.VMEM((parts, N // parts, D), BF16), dma((2 + 2 * parts,))],
            compiler_params=pltpu.CompilerParams(vmem_limit_bytes=VMEM_LIMIT),
        )(lp, hidden_out)
        return lp.reshape(N), hidden_out

    return jax.shard_map(local_step, mesh=mesh, in_specs=in_specs, out_specs=(P(), P()), check_vma=False)
```
